512 devices in a mesh: trial: 4 (over x), span: 16 (over y, core), heads: 8 (over z).
Axes of the slice: x: 4, y: 8, z: 8, core: 2. Of those that a mesh axis runs over, the one named last changes fastest.
Arguments:
- latents: bfloat16 [64, 4096, 512], P('trial', ('span', 'heads')), parts along dimension 0, may hold values from -6 to 6
- rotary_rows: bfloat16 [64, 4096, 64], P('trial', ('span', 'heads')), parts along dimension 0, may hold values from -6 to 6
- latent_gain: float32 [512], replicated, may hold values from 0.25 to 1.75
- key_up: bfloat16 [2048, 16, 128], P('trial', 'heads'), parts along dimension 0, may hold values from -0.25 to 0.25
- value_up: bfloat16 [2048, 16, 128], P('trial', 'heads'), parts along dimension 0, may hold values from -0.25 to 0.25
Outputs:
- cache_keys: bfloat16 [64, 16, 192, 4096], P(('trial', 'span'), 'heads'), parts along dimension 0
- cache_values: bfloat16 [64, 4096, 16, 128], P(('trial', 'span'), None, 'heads'), parts along dimension 0
The draws below stay inside these ranges and needn't reach their ends.
There are 4 independent parts, one for each index of `trial`. The reference program is written for one: setup_inputs(seed, part) draws one part's arguments, and reference() takes and returns one part's arrays. A program takes and returns all parts, laid end to end along the dimension named above; an argument that names none is the same for every part. Nothing has to cross between parts.
All inputs are finite; a program needn't handle non-finite values.
Results may differ from the reference program's by a relative error of at most 0.0049.
Values may be sent and summed in bfloat16 or wider, within the bound.
No kernel may reach another device: no remote copies, remote signals or barrier semaphores. Data moves between devices by JAX's collectives and lax.ppermute only.
A program may use at most 64 MiB of HBM per device.

```python
import jax
import jax.numpy as jnp
from jax import lax

BATCH = 16
LENGTH = 4096
HEADS = 16
LATENT = 512
KEY_PART = 128
ROTARY = 64
VALUE_SIZE = 128


def shard_levels(key, extent, shards, smallest, high):
    level, own = 1.0, jax.random.fold_in(key, 6)
    for dim, blocks in shards:
        steps = jnp.exp(jax.random.uniform(jax.random.fold_in(own, dim), (blocks,), jnp.float32, smallest / len(shards), high / len(shards)))
        level = level * jnp.repeat(steps, extent[dim] // blocks).reshape([-1 if axis == dim else 1 for axis in range(len(extent))])
    return level


def bell_draw(own_key, shape, width, most, cuts=(), kind=jnp.bfloat16):
    values = width * jax.random.normal(own_key, shape, jnp.float32)
    if cuts:
        values = values * shard_levels(own_key, shape, cuts, -0.22, 0.18)
    return jnp.clip(values, -most, most).astype(kind)


def setup_inputs(seed: int = 0, part: int = 0) -> dict:
    seeds = jax.random.split(jax.random.key(seed), 6)
    own_keys = jax.random.split(jax.random.fold_in(seeds[5], part), 6)
    return {
        "latents": bell_draw(own_keys[0], (BATCH, LENGTH, LATENT), 1.0, 6.0, ((1, 128),)),
        "rotary_rows": bell_draw(own_keys[1], (BATCH, LENGTH, ROTARY), 1.0, 6.0, ((1, 128),)),
        "latent_gain": jnp.clip(1.0 + 0.15 * jax.random.normal(seeds[2], (LATENT,), jnp.float32), 0.25, 1.75),
        "key_up": bell_draw(own_keys[3], (LATENT, HEADS, KEY_PART), LATENT ** -0.5, 0.25, ((1, 8),)),
        "value_up": bell_draw(own_keys[4], (LATENT, HEADS, VALUE_SIZE), LATENT ** -0.5, 0.25, ((1, 8),)),
    }


def unit_rows(vectors, row_gain):
    return vectors * lax.rsqrt(lax.optimization_barrier(jnp.mean(vectors * vectors, axis=-1, keepdims=True)) + 1e-06) * row_gain

def reference(latents, rotary_rows, latent_gain, key_up, value_up):
    rows_ready = unit_rows(latents.astype(jnp.float32), latent_gain).astype(jnp.bfloat16)
    rows_ready = lax.optimization_barrier(rows_ready)

    def expand_one(one):
        rows_one, rotary_one = one
        wide_keys = jnp.einsum('tr,rhk->thk', rows_one.astype(jnp.float32), key_up.astype(jnp.float32)).astype(jnp.bfloat16)
        shared = jnp.broadcast_to(rotary_one[:, None], (LENGTH, HEADS, ROTARY))
        wide_values = jnp.einsum('tr,rhk->thk', rows_one.astype(jnp.float32), value_up.astype(jnp.float32)).astype(jnp.bfloat16)
        return (jnp.concatenate([wide_keys, shared], axis=-1), wide_values)
    cache_keys, cache_values = lax.map(expand_one, (rows_ready, rotary_rows))
    cache_keys = jnp.transpose(cache_keys, (0, 2, 3, 1))
    return (cache_keys, cache_values)
```

```python
import functools

import jax
import jax.numpy as jnp
from jax import lax
from jax.experimental import pallas as pl
from jax.experimental.pallas import tpu as pltpu
from jax.sharding import PartitionSpec as P

CHUNKS = 2


def pack_kernel(lat_ref, rot_ref, gain_ref, out_ref):
    x = lat_ref[...].astype(jnp.float32)
    scale = lax.rsqrt(jnp.mean(x * x, axis=-1, keepdims=True) + 1e-06)
    rows = (x * scale * gain_ref[...][None]).astype(jnp.bfloat16)
    n, width = x.shape[1], x.shape[2]
    for j in range(width // 128):
        out_ref[:, j * n : (j + 1) * n, :] = rows[:, :, j * 128 : (j + 1) * 128]
    base, half = (width // 128) * n, n // 2
    rot = rot_ref[...]
    out_ref[:, base : base + half, 0:64] = rot[:, :half]
    out_ref[:, base : base + half, 64:128] = rot[:, half:]


def pack(latents, rotary, gain):
    s, n, width = latents.shape
    return pl.pallas_call(
        pack_kernel,
        out_shape=jax.ShapeDtypeStruct((s, n * (width + 64) // 128, 128), jnp.bfloat16),
        name="pack",
    )(latents, rotary, gain.reshape(1, width))


def expand_kernel(z_ref, wk_ref, wv_ref, *refs, zs, n, width, first):
    x_refs = refs[:zs]
    keys_ref, vals_ref, rows_s, rot_s = refs[zs + (0 if first else 2) :]
    z = z_ref[0]
    per = zs * n
    sps = x_refs[0].shape[0]
    half = n // 2
    base = (width // 128) * n
    for s in range(sps):
        for k, x_ref in enumerate(x_refs):
            at = pl.multiple_of(s * per + lax.rem(z + zs - k, zs) * n, n)
            for j in range(width // 128):
                rows_s[pl.ds(at, n), j * 128 : (j + 1) * 128] = x_ref[s, j * n : (j + 1) * n, :]
            rot_s[pl.ds(at, half), :] = x_ref[s, base : base + half, 0:64]
            rot_s[pl.ds(at + half, half), :] = x_ref[s, base : base + half, 64:128]
    ri = lax.broadcasted_iota(jnp.int32, (256, 256), 0)
    ci = lax.broadcasted_iota(jnp.int32, (256, 256), 1)
    target = jnp.where(ci < 128, 2 * ci, 2 * ci - 255)
    weave = (ri == target).astype(jnp.bfloat16)
    for s in range(sps):
        r = rows_s[s * per : (s + 1) * per, :]
        kt = lax.dot_general(
            wk_ref[...], r, (((1,), (1,)), ((), ())), preferred_element_type=jnp.float32
        ).astype(jnp.bfloat16)
        rt = rot_s[s * per : (s + 1) * per, :].T
        for h in range(2):
            keys_ref[h, 0:128, s * per : (s + 1) * per] = kt[h * 128 : (h + 1) * 128]
            keys_ref[h, 128:192, s * per : (s + 1) * per] = rt
        v = jnp.dot(r, wv_ref[...], preferred_element_type=jnp.float32).astype(jnp.bfloat16)
        for b in range(per // 128):
            both = jnp.concatenate(
                [v[b * 128 : (b + 1) * 128, :128], v[b * 128 : (b + 1) * 128, 128:]], axis=0
            )
            m = jnp.dot(weave, both, preferred_element_type=jnp.float32).astype(jnp.bfloat16)
            at = (s * per + b * 128) * 2
            vals_ref[at : at + 256, :] = m


def expand(z, wk, wv, slots, offset, length, prev, sp_step=2):
    zs = len(slots)
    sps, packed, _ = slots[0].shape
    width = wk.shape[1]
    n = packed * 128 // (width + 64)
    per = zs * n
    steps = sps // sp_step
    off = offset // sp_step
    first = prev is None
    kshape = jax.ShapeDtypeStruct((2, 192, length), jnp.bfloat16)
    vshape = jax.ShapeDtypeStruct((2 * length, 128), jnp.bfloat16)
    in_specs = [
        pl.BlockSpec(memory_space=pltpu.SMEM),
        pl.BlockSpec(wk.shape, lambda i: (0, 0)),
        pl.BlockSpec(wv.shape, lambda i: (0, 0)),
    ] + [pl.BlockSpec((sp_step, packed, 128), lambda i: (i, 0, 0)) for _ in slots]
    args = [z, wk, wv, *slots]
    aliases = {}
    if not first:
        aliases = {len(args): 0, len(args) + 1: 1}
        in_specs += [pl.BlockSpec(memory_space=pl.ANY)] * 2
        args += list(prev)
    return pl.pallas_call(
        functools.partial(expand_kernel, zs=zs, n=n, width=width, first=first),
        grid=(steps,),
        in_specs=in_specs,
        out_specs=[
            pl.BlockSpec((2, 192, sp_step * per), lambda i: (0, 0, i + off)),
            pl.BlockSpec((sp_step * per * 2, 128), lambda i: (i + off, 0)),
        ],
        out_shape=[kshape, vshape],
        scratch_shapes=[
            pltpu.VMEM((sp_step * per, width), jnp.bfloat16),
            pltpu.VMEM((sp_step * per, 64), jnp.bfloat16),
        ],
        input_output_aliases=aliases,
        name="expand",
    )(*args)


def ring(chunks, axis):
    n = lax.axis_size(axis)
    right = [(i, (i + 1) % n) for i in range(n)]
    left = [(i, (i - 1) % n) for i in range(n)]
    slots = [[x] + [None] * (n - 1) for x in chunks]
    for step in range(1, n // 2 + 1):
        for c in range(len(chunks)):
            if step < n // 2 or c % 2 == 0:
                slots[c][step] = lax.ppermute(slots[c][step - 1], axis, right)
            if step < n // 2 or c % 2 == 1:
                slots[c][n - step] = lax.ppermute(slots[c][(n - step + 1) % n], axis, left)
    return slots


def shards(latents, rotary_rows, latent_gain, key_up, value_up):
    width = latents.shape[2]
    packed = pack(latents, rotary_rows, latent_gain)
    moved = lax.all_to_all(packed, "span", split_axis=0, concat_axis=0, tiled=True)
    spans = moved.shape[0]
    each = spans // CHUNKS
    slots = ring([moved[c * each : (c + 1) * each] for c in range(CHUNKS)], "heads")
    wk = key_up.reshape(width, -1).T
    wv = value_up.reshape(width, -1)
    z = lax.axis_index("heads").astype(jnp.int32).reshape(1)
    length = spans * lax.axis_size("heads") * latents.shape[1]
    outs = None
    for c in range(CHUNKS):
        outs = expand(z, wk, wv, slots[c], c * each, length, outs)
    keys, vals = outs
    return (keys[None], vals.reshape(1, length, 2, 128))


def solution(mesh):
    return jax.shard_map(
        shards,
        mesh=mesh,
        in_specs=(
            P("trial", ("span", "heads"), None),
            P("trial", ("span", "heads"), None),
            P(),
            P("trial", "heads", None),
            P("trial", "heads", None),
        ),
        out_specs=(
            P(("trial", "span"), "heads", None, None),
            P(("trial", "span"), None, "heads", None),
        ),
        check_vma=False,
    )
```
